256 devices in a mesh: row: 16 (over z_lo, x), col: 4 (over z_hi, core), depth: 4 (over y).
Axes of the slice: x: 4, y: 4, z: 8 (z_hi: 2, z_lo: 4; z = z_hi * 4 + z_lo), core: 2. Of those that a mesh axis runs over, the one named last changes fastest.
Arguments:
- inputs: bfloat16 [1024, 5120], P(('row', 'depth'), 'col'), may hold values from -6 to 6
- targets: bfloat16 [1024, 5120], P(('row', 'depth'), 'col'), may hold values from -6 to 6
- norm_gain: float32 [5120], P('col'), may hold values from 0.5 to 1.5
- w_gate: bfloat16 [5120, 8192], P('col', ('row', 'depth')), may hold values from -0.078125 to 0.078125
- w_up: bfloat16 [5120, 8192], P('col', ('row', 'depth')), may hold values from -0.078125 to 0.078125
- w_down: bfloat16 [8192, 5120], P(('row', 'depth'), 'col'), may hold values from -0.0625 to 0.0625
- probe_gate: bfloat16 [5120, 8192], P('col', ('row', 'depth')), may hold values from -1 to 1, as said below
- probe_up: bfloat16 [5120, 8192], P('col', ('row', 'depth')), may hold values from -1 to 1, as said below
- probe_down: bfloat16 [8192, 5120], P(('row', 'depth'), 'col'), may hold values from -1 to 1, as said below
- moment_gate: float32 [5120, 8192], P('col', ('row', 'depth')), may hold values from -18 to 18
- moment_up: float32 [5120, 8192], P('col', ('row', 'depth')), may hold values from -18 to 18
- moment_down: float32 [8192, 5120], P(('row', 'depth'), 'col'), may hold values from -18 to 18
- second_gate: float32 [5120, 8192], P('col', ('row', 'depth')), may hold values from 1 to 100
- second_up: float32 [5120, 8192], P('col', ('row', 'depth')), may hold values from 1 to 100
- second_down: float32 [8192, 5120], P(('row', 'depth'), 'col'), may hold values from 1 to 100
Outputs:
- new_moment_gate: float32 [5120, 8192], P('col', ('row', 'depth'))
- new_moment_up: float32 [5120, 8192], P('col', ('row', 'depth'))
- new_moment_down: float32 [8192, 5120], P(('row', 'depth'), 'col')
- new_second_gate: float32 [5120, 8192], P('col', ('row', 'depth'))
- new_second_up: float32 [5120, 8192], P('col', ('row', 'depth'))
- new_second_down: float32 [8192, 5120], P(('row', 'depth'), 'col')
- step_gate: float32 [5120, 8192], P('col', ('row', 'depth'))
- step_up: float32 [5120, 8192], P('col', ('row', 'depth'))
- step_down: float32 [8192, 5120], P(('row', 'depth'), 'col')
The draws below stay inside these ranges and needn't reach their ends.
Inputs may be any that keep to these rules, and one draw needn't show every extreme that they name: `probe_gate`: every entry is +1 or -1. `probe_up`: every entry is +1 or -1. `probe_down`: every entry is +1 or -1.
All inputs are finite; a program needn't handle non-finite values.
Results may differ from the reference program's by a relative error of at most 0.0046.
Values may be sent and summed in bfloat16 or wider, within the bound.
No kernel may reach another device: no remote copies, remote signals or barrier semaphores. Data moves between devices by JAX's collectives and lax.ppermute only.
A program may use at most 128 MiB of HBM per device.

```python
import math
import jax
import jax.numpy as jnp
from jax import lax

D = 5120
FF = 8192
TILE = 128
STEP = 1000
TOKENS = 1024


def rademacher(key, height, breadth):
    coins = jax.random.randint(key, (height, breadth), 0, 2)
    return (2.0 * coins.astype(jnp.float32) - 1.0).astype(jnp.bfloat16)


def draw_probe_gate(key, part):
    return rademacher(jax.random.fold_in(key, 101), D, FF)


def draw_probe_up(key, part):
    return rademacher(jax.random.fold_in(key, 202), D, FF)


def draw_probe_down(key, part):
    return rademacher(jax.random.fold_in(key, 303), FF, D)


def shard_levels(key, extent, cuts, low, high):
    factor_of = 1.0
    for axis_at, parts in cuts:
        heights = jax.random.uniform(jax.random.fold_in(jax.random.fold_in(key, 6), axis_at), (parts,), jnp.float32, low / len(cuts), high / len(cuts))
        factor_of = factor_of * jnp.repeat(jnp.exp(heights), extent[axis_at] // parts).reshape((-1,) + (1,) * (len(extent) - 1 - axis_at))
    return factor_of


def gaussian(key, extent, spread, reach, pieces=(), kind=jnp.bfloat16):
    loudness = shard_levels(key, extent, pieces, -0.22, 0.18) if pieces else 1.0
    array = jax.random.normal(key, extent, jnp.float32) * spread * loudness
    return jnp.minimum(jnp.maximum(array, -reach), reach).astype(kind)


def setup_inputs(seed: int = 0) -> dict:
    seeds = jax.random.split(jax.random.key(seed), 16)
    inputs = gaussian(seeds[0], (TOKENS, D), 1.0, 6.0, ((0, 64), (1, 4)))
    targets = gaussian(seeds[1], (TOKENS, D), 1.0, 6.0, ((0, 64), (1, 4)))
    norm_gain = jnp.clip(1.0 + 0.1 * jax.random.normal(seeds[2], (D,), jnp.float32), 0.5, 1.5)
    w_gate = gaussian(seeds[3], (D, FF), D ** -0.5, 0.078125, ((0, 4), (1, 64)))
    w_up = gaussian(seeds[4], (D, FF), D ** -0.5, 0.078125, ((0, 4), (1, 64)))
    w_down = gaussian(seeds[5], (FF, D), FF ** -0.5, 0.0625, ((0, 64), (1, 4)))
    probe_gate = draw_probe_gate(jax.random.fold_in(seeds[15], 71), 0)
    probe_up = draw_probe_up(jax.random.fold_in(seeds[15], 71), 0)
    probe_down = draw_probe_down(jax.random.fold_in(seeds[15], 71), 0)
    moment_gate = gaussian(seeds[9], (D, FF), 3.0, 18.0, ((0, 4), (1, 64)), jnp.float32)
    moment_up = gaussian(seeds[10], (D, FF), 3.0, 18.0, ((0, 4), (1, 64)), jnp.float32)
    moment_down = gaussian(seeds[11], (FF, D), 3.0, 18.0, ((0, 64), (1, 4)), jnp.float32)
    second_gate = jnp.clip(jnp.exp(math.log(100.0) - 4.6051702 * jax.random.uniform(seeds[12], (D, FF), jnp.float32) ** shard_levels(seeds[12], (D, FF), ((0, 4), (1, 64)), -0.2, 0.2)), 1.0, 100.0)
    second_up = jnp.clip(jnp.exp(math.log(100.0) - 4.6051702 * jax.random.uniform(seeds[13], (D, FF), jnp.float32) ** shard_levels(seeds[13], (D, FF), ((0, 4), (1, 64)), -0.2, 0.2)), 1.0, 100.0)
    second_down = jnp.clip(jnp.exp(math.log(100.0) - 4.6051702 * jax.random.uniform(seeds[14], (FF, D), jnp.float32) ** shard_levels(seeds[14], (FF, D), ((0, 64), (1, 4)), -0.2, 0.2)), 1.0, 100.0)
    return {"inputs": inputs, "targets": targets, "norm_gain": norm_gain, "w_gate": w_gate, "w_up": w_up, "w_down": w_down, "probe_gate": probe_gate, "probe_up": probe_up, "probe_down": probe_down, "moment_gate": moment_gate, "moment_up": moment_up, "moment_down": moment_down, "second_gate": second_gate, "second_up": second_up, "second_down": second_down}


beta_one = 0.9
beta_two = 0.999
adam_floor = 1e-08
norm_floor = 1e-05

def silu_parts(gate_pre):
    sig = jax.nn.sigmoid(gate_pre)
    act = gate_pre * sig
    slope = sig * (1.0 + gate_pre * (1.0 - sig))
    bend = sig * (1.0 - sig) * (2.0 + gate_pre * (1.0 - 2.0 * sig))
    return (act, slope, bend)

def tile_means(product):
    height, breadth = product.shape
    blocks = product.reshape(height // TILE, TILE, breadth // TILE, TILE)
    means = lax.optimization_barrier(jnp.mean(blocks, axis=(1, 3), keepdims=True))
    return jnp.broadcast_to(means, blocks.shape).reshape(height, breadth)

def adahessian(moment, second, gradient, curvature, probe):
    averaged = tile_means(probe.astype(jnp.float32) * curvature)
    new_moment = beta_one * moment + (1.0 - beta_one) * gradient
    new_second = beta_two * second + (1.0 - beta_two) * averaged * averaged
    corrected = new_moment / (1.0 - beta_one ** STEP)
    scale_root = jnp.sqrt(new_second / (1.0 - beta_two ** STEP))
    return (new_moment, new_second, corrected / (scale_root + adam_floor))

def matmul(left, right):
    return jnp.dot(left, right, preferred_element_type=jnp.float32)

def inner_left(left, right):
    return lax.dot_general(left, right, (((0,), (0,)), ((), ())), preferred_element_type=jnp.float32)

def inner_right(left, right):
    return lax.dot_general(left, right, (((1,), (1,)), ((), ())), preferred_element_type=jnp.float32)

def reference(inputs, targets, norm_gain, w_gate, w_up, w_down, probe_gate, probe_up, probe_down, moment_gate, moment_up, moment_down, second_gate, second_up, second_down):
    feats = inputs.astype(jnp.float32)
    meansq = lax.optimization_barrier(jnp.mean(feats * feats, axis=1, keepdims=True))
    normed = (feats * lax.rsqrt(meansq + norm_floor) * norm_gain).astype(jnp.bfloat16)
    gate_pre = matmul(normed, w_gate)
    up_pre = matmul(normed, w_up)
    gate_tan = matmul(normed, probe_gate)
    up_tan = matmul(normed, probe_up)
    act, slope, bend = silu_parts(gate_pre)
    hidden = (act * up_pre).astype(jnp.bfloat16)
    hidden_tan = (slope * gate_tan * up_pre + act * up_tan).astype(jnp.bfloat16)
    outputs = feats + matmul(hidden, w_down)
    error = (outputs - targets.astype(jnp.float32)).astype(jnp.bfloat16)
    error_tan = (matmul(hidden_tan, w_down) + matmul(hidden, probe_down)).astype(jnp.bfloat16)
    back_hidden = inner_right(error, w_down)
    back_tan = inner_right(error_tan, w_down) + inner_right(error, probe_down)
    back_gate = (back_hidden * up_pre * slope).astype(jnp.bfloat16)
    back_up = (back_hidden * act).astype(jnp.bfloat16)
    gate_tan_back = (back_tan * up_pre * slope + back_hidden * up_tan * slope + back_hidden * up_pre * bend * gate_tan).astype(jnp.bfloat16)
    up_tan_back = (back_tan * act + back_hidden * slope * gate_tan).astype(jnp.bfloat16)
    grad_gate = inner_left(normed, back_gate)
    grad_up = inner_left(normed, back_up)
    grad_down = inner_left(hidden, error)
    curve_gate = inner_left(normed, gate_tan_back)
    curve_up = inner_left(normed, up_tan_back)
    curve_down = inner_left(hidden_tan, error) + inner_left(hidden, error_tan)
    gate_moment, gate_second, gate_step = adahessian(moment_gate, second_gate, grad_gate, curve_gate, probe_gate)
    up_moment, up_second, up_step = adahessian(moment_up, second_up, grad_up, curve_up, probe_up)
    down_moment, down_second, down_step = adahessian(moment_down, second_down, grad_down, curve_down, probe_down)
    return (gate_moment, up_moment, down_moment, gate_second, up_second, down_second, gate_step, up_step, down_step)
```

```python
import jax
import jax.numpy as jnp
from jax import lax
from jax.sharding import Mesh
from jax.sharding import PartitionSpec as P

D = 5120
TILE = 128
STEP = 1000

beta_one = 0.9
beta_two = 0.999
adam_floor = 1e-08
norm_floor = 1e-05

RING = 4
BF = jnp.bfloat16
F32 = jnp.float32


def shifted(value, axis, shift):
    count = lax.axis_size(axis)
    return lax.ppermute(value, axis, [(i, (i + shift) % count) for i in range(count)])


def gathered(value, axis):
    return jnp.concatenate(
        [value] + [shifted(value, axis, s) for s in range(1, RING)], axis=0
    )


def returned(blocks, axis):
    total = blocks[0].astype(F32)
    for s in range(1, RING):
        total = total + shifted(blocks[s].astype(BF), axis, -s).astype(F32)
    return total


def row_blocks(value):
    height = value.shape[0] // RING
    return [value[s * height : (s + 1) * height] for s in range(RING)]


def gather_rows(value, axes):
    for axis in axes:
        value = gathered(value, axis)
    return value


def swapped(value, axis):
    return lax.ppermute(value, axis, [(0, 1), (1, 0)])


def sum_over_col(value):
    half = value.shape[0] // 2
    me = lax.axis_index("c")
    low, high = value[:half], value[half:]
    keep = jnp.where(me == 0, low, high)
    give = jnp.where(me == 0, high, low).astype(BF)
    mine = keep + swapped(give, "c").astype(F32)
    mine = mine + swapped(mine.astype(BF), "zh").astype(F32)
    other = swapped(mine.astype(BF), "c").astype(F32)
    return jnp.concatenate(
        [jnp.where(me == 0, mine, other), jnp.where(me == 0, other, mine)], axis=0
    )


def silu_parts(gate_pre):
    sig = jax.nn.sigmoid(gate_pre)
    act = gate_pre * sig
    slope = sig * (1.0 + gate_pre * (1.0 - sig))
    bend = sig * (1.0 - sig) * (2.0 + gate_pre * (1.0 - 2.0 * sig))
    return (act, slope, bend)


def tile_means(product):
    height, breadth = product.shape
    blocks = product.reshape(height // TILE, TILE, breadth // TILE, TILE)
    means = jnp.mean(blocks, axis=(1, 3), keepdims=True)
    return jnp.broadcast_to(means, blocks.shape).reshape(height, breadth)


def adahessian(moment, second, gradient, curvature, probe):
    averaged = tile_means(probe.astype(F32) * curvature)
    new_moment = beta_one * moment + (1.0 - beta_one) * gradient
    new_second = beta_two * second + (1.0 - beta_two) * averaged * averaged
    corrected = new_moment / (1.0 - beta_one**STEP)
    scale_root = jnp.sqrt(new_second / (1.0 - beta_two**STEP))
    return (new_moment, new_second, corrected / (scale_root + adam_floor))


def matmul(left, right):
    return jnp.dot(left, right, preferred_element_type=F32)


def inner_left(left, right):
    return lax.dot_general(
        left, right, (((0,), (0,)), ((), ())), preferred_element_type=F32
    )


def inner_right(left, right):
    return lax.dot_general(
        left, right, (((1,), (1,)), ((), ())), preferred_element_type=F32
    )


def chunk_forward_and_back(inputs, targets, first_weights, w_down, both_down, axes):
    width = inputs.shape[1]
    block = w_down.shape[0]
    x = gather_rows(inputs, ("zl",) + axes)
    x32 = x.astype(F32)
    squares = jnp.sum(x32 * x32, axis=1)
    squares = squares + swapped(squares, "c")
    squares = squares + swapped(squares, "zh")
    scale = lax.rsqrt(squares / D + norm_floor)[:, None]

    projected = sum_over_col(matmul(x, first_weights)) * scale
    gate_pre, up_pre, gate_tan, up_tan = (
        projected[:, k * block : (k + 1) * block] for k in range(4)
    )
    act, slope, bend = silu_parts(gate_pre)
    hidden = (act * up_pre).astype(BF)
    hidden_tan = (slope * gate_tan * up_pre + act * up_tan).astype(BF)
    both = jnp.concatenate([hidden_tan, hidden], axis=1)

    terms = [
        jnp.concatenate([matmul(h, w_down), matmul(b, both_down)], axis=1)
        for h, b in zip(row_blocks(hidden), row_blocks(both))
    ]
    summed = returned(terms, axes[1])
    summed = returned(row_blocks(summed), axes[0])
    summed = returned(row_blocks(summed), "zl")
    outputs = summed[:, :width] + inputs.astype(F32)
    error_rows = (outputs - targets.astype(F32)).astype(BF)
    tangent_rows = summed[:, width:].astype(BF)
    errors = gather_rows(
        jnp.concatenate([error_rows, tangent_rows], axis=1), ("zl",) + axes
    )
    error, error_tan = errors[:, :width], errors[:, width:]

    back = sum_over_col(
        jnp.concatenate(
            [
                inner_right(error, w_down),
                inner_right(error_tan, w_down)
                + inner_right(error, both_down[block:]),
            ],
            axis=1,
        )
    )
    back_hidden, back_tan = back[:, :block], back[:, block:]
    back_gate = back_hidden * up_pre * slope
    back_up = back_hidden * act
    gate_tan_back = (
        back_tan * up_pre * slope
        + back_hidden * up_tan * slope
        + back_hidden * up_pre * bend * gate_tan
    )
    up_tan_back = back_tan * act + back_hidden * slope * gate_tan
    backs = (
        jnp.concatenate([back_gate, back_up, gate_tan_back, up_tan_back], axis=1)
        * scale
    ).astype(BF)
    first = inner_left(x, backs)
    grad_down = inner_left(hidden, error)
    curve_down = inner_left(hidden_tan, error) + inner_left(hidden, error_tan)
    return first, grad_down, curve_down


def shards(
    inputs,
    targets,
    norm_gain,
    w_gate,
    w_up,
    w_down,
    probe_gate,
    probe_up,
    probe_down,
    moment_gate,
    moment_up,
    moment_down,
    second_gate,
    second_up,
    second_down,
):
    block = w_gate.shape[1]
    rows = inputs.shape[0]
    gain = norm_gain[:, None]
    first_weights = (
        gain
        * jnp.concatenate([w_gate, w_up, probe_gate, probe_up], axis=1).astype(F32)
    ).astype(BF)
    both_down = jnp.concatenate([w_down, probe_down], axis=0)
    parts = []
    for k, axes in enumerate((("y", "x"), ("x", "y"))):
        low, high = k * rows // 2, (k + 1) * rows // 2
        parts.append(
            chunk_forward_and_back(
                inputs[low:high], targets[low:high], first_weights, w_down, both_down, axes
            )
        )
    first, grad_down, curve_down = (a + b for a, b in zip(*parts))
    first = gain * first
    grad_gate, grad_up, curve_gate, curve_up = (
        first[:, k * block : (k + 1) * block] for k in range(4)
    )
    gate_moment, gate_second, gate_step = adahessian(
        moment_gate, second_gate, grad_gate, curve_gate, probe_gate
    )
    up_moment, up_second, up_step = adahessian(
        moment_up, second_up, grad_up, curve_up, probe_up
    )
    down_moment, down_second, down_step = adahessian(
        moment_down, second_down, grad_down, curve_down, probe_down
    )
    return (
        gate_moment,
        up_moment,
        down_moment,
        gate_second,
        up_second,
        down_second,
        gate_step,
        up_step,
        down_step,
    )


def solution(mesh):
    grid = Mesh(mesh.devices.reshape(4, 4, 2, 2, 4), ("zl", "x", "zh", "c", "y"))
    tokens, feats = ("zl", "x", "y"), ("zh", "c")
    rows, tall, wide = P(tokens, feats), P(feats, tokens), P(tokens, feats)
    return jax.shard_map(
        shards,
        mesh=grid,
        in_specs=(rows, rows, P(feats)) + (tall, tall, wide) * 4,
        out_specs=(tall, tall, wide) * 3,
        check_vma=False,
    )
```

```python
import jax
import jax.numpy as jnp
from jax import lax
from jax.sharding import Mesh
from jax.sharding import PartitionSpec as P

D = 5120
TILE = 128
STEP = 1000

beta_one = 0.9
beta_two = 0.999
adam_floor = 1e-08
norm_floor = 1e-05

RING = 4
BF = jnp.bfloat16
F32 = jnp.float32


def shifted(value, axis, shift):
    count = lax.axis_size(axis)
    return lax.ppermute(value, axis, [(i, (i + shift) % count) for i in range(count)])


def gathered(value, axis):
    return jnp.concatenate(
        [value] + [shifted(value, axis, s) for s in range(1, RING)], axis=0
    )


def returned(blocks, axis):
    total = blocks[0].astype(F32)
    for s in range(1, RING):
        total = total + shifted(blocks[s].astype(BF), axis, -s).astype(F32)
    return total


def row_blocks(value):
    height = value.shape[0] // RING
    return [value[s * height : (s + 1) * height] for s in range(RING)]


def gather_rows(value, axes):
    for axis in axes:
        value = gathered(value, axis)
    return value


def swapped(value, axis):
    return lax.ppermute(value, axis, [(0, 1), (1, 0)])


def sum_over_col(value):
    half = value.shape[0] // 2
    me = lax.axis_index("c")
    low, high = value[:half], value[half:]
    keep = jnp.where(me == 0, low, high)
    give = jnp.where(me == 0, high, low)
    mine = keep + swapped(give, "c")
    mine = mine + swapped(mine.astype(BF), "zh").astype(F32)
    other = swapped(mine, "c")
    return jnp.concatenate(
        [jnp.where(me == 0, mine, other), jnp.where(me == 0, other, mine)], axis=0
    )


def silu_parts(gate_pre):
    sig = jax.nn.sigmoid(gate_pre)
    act = gate_pre * sig
    slope = sig * (1.0 + gate_pre * (1.0 - sig))
    bend = sig * (1.0 - sig) * (2.0 + gate_pre * (1.0 - 2.0 * sig))
    return (act, slope, bend)


def tile_means(product):
    height, breadth = product.shape
    blocks = product.reshape(height // TILE, TILE, breadth // TILE, TILE)
    means = jnp.mean(blocks, axis=(1, 3), keepdims=True)
    return jnp.broadcast_to(means, blocks.shape).reshape(height, breadth)


def adahessian(moment, second, gradient, curvature, probe):
    averaged = tile_means(probe.astype(F32) * curvature)
    new_moment = beta_one * moment + (1.0 - beta_one) * gradient
    new_second = beta_two * second + (1.0 - beta_two) * averaged * averaged
    corrected = new_moment / (1.0 - beta_one**STEP)
    scale_root = jnp.sqrt(new_second / (1.0 - beta_two**STEP))
    return (new_moment, new_second, corrected / (scale_root + adam_floor))


def matmul(left, right):
    return jnp.dot(left, right, preferred_element_type=F32)


def inner_left(left, right):
    return lax.dot_general(
        left, right, (((0,), (0,)), ((), ())), preferred_element_type=F32
    )


def inner_right(left, right):
    return lax.dot_general(
        left, right, (((1,), (1,)), ((), ())), preferred_element_type=F32
    )


def chunk_forward_and_back(normed, inputs, targets, firsts, w_down, probe_down, axes):
    width = inputs.shape[1]
    block = w_down.shape[0]
    x = gather_rows(normed, axes)
    projected = sum_over_col(
        jnp.concatenate([matmul(x, w) for w in firsts], axis=1)
    )
    gate_pre, up_pre, gate_tan, up_tan = (
        projected[:, k * block : (k + 1) * block] for k in range(4)
    )
    act, slope, bend = silu_parts(gate_pre)
    hidden = (act * up_pre).astype(BF)
    hidden_tan = (slope * gate_tan * up_pre + act * up_tan).astype(BF)

    terms = [
        jnp.concatenate(
            [matmul(h, w_down), matmul(t, w_down) + matmul(h, probe_down)], axis=1
        )
        for h, t in zip(row_blocks(hidden), row_blocks(hidden_tan))
    ]
    summed = returned(terms, axes[1])
    summed = returned(row_blocks(summed), axes[0])
    summed = returned(row_blocks(summed), "zl")
    outputs = summed[:, :width] + inputs.astype(F32)
    error_rows = (outputs - targets.astype(F32)).astype(BF)
    tangent_rows = summed[:, width:].astype(BF)
    errors = gather_rows(
        jnp.concatenate([error_rows, tangent_rows], axis=1), ("zl",) + axes
    )
    error, error_tan = errors[:, :width], errors[:, width:]

    back = sum_over_col(
        jnp.concatenate(
            [
                inner_right(error, w_down),
                inner_right(error_tan, w_down) + inner_right(error, probe_down),
            ],
            axis=1,
        )
    )
    back_hidden, back_tan = back[:, :block], back[:, block:]
    back_gate = (back_hidden * up_pre * slope).astype(BF)
    back_up = (back_hidden * act).astype(BF)
    gate_tan_back = (
        back_tan * up_pre * slope
        + back_hidden * up_tan * slope
        + back_hidden * up_pre * bend * gate_tan
    ).astype(BF)
    up_tan_back = (back_tan * act + back_hidden * slope * gate_tan).astype(BF)
    return (
        inner_left(x, back_gate),
        inner_left(x, back_up),
        inner_left(x, gate_tan_back),
        inner_left(x, up_tan_back),
        inner_left(hidden, error),
        inner_left(hidden_tan, error) + inner_left(hidden, error_tan),
    )


def normed_rows(inputs, norm_gain):
    feats = inputs.astype(F32)
    mine = jnp.sum(feats * feats, axis=1)
    both = ("zh", "c")
    squares = mine
    for s in range(1, RING):
        squares = squares + lax.ppermute(mine, both, [(i, i ^ s) for i in range(RING)])
    scaling = lax.rsqrt(squares / D + norm_floor)
    return (feats * scaling[:, None] * norm_gain).astype(BF)


def shards(
    inputs,
    targets,
    norm_gain,
    w_gate,
    w_up,
    w_down,
    probe_gate,
    probe_up,
    probe_down,
    moment_gate,
    moment_up,
    moment_down,
    second_gate,
    second_up,
    second_down,
):
    rows = inputs.shape[0]
    half = rows // 2
    width = inputs.shape[1]
    layered = gathered(normed_rows(inputs, norm_gain), "zl").reshape(RING, rows, width)
    parts = []
    for k, axes in enumerate((("y", "x"), ("x", "y"))):
        low, high = k * half, (k + 1) * half
        parts.append(
            chunk_forward_and_back(
                layered[:, low:high].reshape(RING * half, width),
                inputs[low:high],
                targets[low:high],
                (w_gate, w_up, probe_gate, probe_up),
                w_down,
                probe_down,
                axes,
            )
        )
    grad_gate, grad_up, curve_gate, curve_up, grad_down, curve_down = (
        a + b for a, b in zip(*parts)
    )
    gate_moment, gate_second, gate_step = adahessian(
        moment_gate, second_gate, grad_gate, curve_gate, probe_gate
    )
    up_moment, up_second, up_step = adahessian(
        moment_up, second_up, grad_up, curve_up, probe_up
    )
    down_moment, down_second, down_step = adahessian(
        moment_down, second_down, grad_down, curve_down, probe_down
    )
    return (
        gate_moment,
        up_moment,
        down_moment,
        gate_second,
        up_second,
        down_second,
        gate_step,
        up_step,
        down_step,
    )


def solution(mesh):
    grid = Mesh(mesh.devices.reshape(4, 4, 2, 2, 4), ("zl", "x", "zh", "c", "y"))
    tokens, feats = ("zl", "x", "y"), ("zh", "c")
    rows, tall, wide = P(tokens, feats), P(feats, tokens), P(tokens, feats)
    return jax.shard_map(
        shards,
        mesh=grid,
        in_specs=(rows, rows, P(feats)) + (tall, tall, wide) * 4,
        out_specs=(tall, tall, wide) * 3,
        check_vma=False,
    )
```
